32 devices in a mesh: dp: 2 (over x), expert: 16 (over z, y, core).
Axes of the slice: x: 2, y: 2, z: 4, core: 2. Of those that a mesh axis runs over, the one named last changes fastest.
Arguments:
- tokens: bfloat16 [256, 2048], P(('dp', 'expert')), may hold values from -6 to 6
- out_grad: bfloat16 [256, 2048], P(('dp', 'expert')), may hold values from -6 to 6
- expert_ids: int32 [256, 8], P(('dp', 'expert')), may hold values from 0 to 15, all different within a row; in each aligned block of 8 rows (0 to 7, 8 to 15, ...) at most 8 rows name the same one
- gate_values: float32 [256, 8], P(('dp', 'expert')), may hold values from 0.05 to 1
- w_gate: bfloat16 [16, 2048, 1024], P('expert', None, 'dp'), may hold values from -0.125 to 0.125
- w_up: bfloat16 [16, 2048, 1024], P('expert', None, 'dp'), may hold values from -0.125 to 0.125
- w_down: bfloat16 [16, 1024, 2048], P('expert', 'dp'), may hold values from -0.1875 to 0.1875
Outputs:
- grad_tokens: bfloat16 [256, 2048], P(('dp', 'expert'))
- grad_gate: float32 [16, 2048, 1024], P('expert', None, 'dp')
- grad_up: float32 [16, 2048, 1024], P('expert', None, 'dp')
- grad_down: float32 [16, 1024, 2048], P('expert', 'dp')
The draws below stay inside these ranges and needn't reach their ends.
Inputs may be any that keep to these rules, and one draw needn't show every extreme that they name: `expert_ids`: each token names 8 different experts. Among the 8 tokens of one device (aligned blocks of 8 rows) no expert is named more than 8 times, and in every draw some expert is named exactly 8 times in some block.
All inputs are finite; a program needn't handle non-finite values.
Results may differ from the reference program's by a relative error of at most 0.014.
Values may be sent and summed in bfloat16 or wider, within the bound.
No kernel may reach another device: no remote copies, remote signals or barrier semaphores. Data moves between devices by JAX's collectives and lax.ppermute only.
A program may use at most 64 MiB of HBM per device.

```python
import math
import jax
import jax.numpy as jnp
import numpy as np
from jax import lax

D = 2048
FF = 1024
TOP = 8
TOK_DEV = 8
EXPERTS = 16
CAP = 8
ROWS = 256
TOKENS = 256
N_DP = 2
N_EXPERT = 16


def steps_of(stream_key, extent, split, least, high):
    def one(dim, blocks):
        heights = jax.random.uniform(jax.random.fold_in(jax.random.fold_in(stream_key, 6), dim), (blocks,), jnp.float32, least / len(split), high / len(split))
        return jnp.repeat(jnp.exp(heights), extent[dim] // blocks).reshape((-1,) + (1,) * (len(extent) - dim - 1))

    factor_of = one(*split[0])
    for cut in split[1:]:
        factor_of = factor_of * one(*cut)
    return factor_of


def routed_block(own_key, own, number, rows, count, top, limit, lean):
    order = jax.random.permutation(own_key, count)
    heavy_load, ordinary = shares(count, rows * top, limit, lean, True), shares(count, rows * top, limit, lean, False)
    places = jnp.arange(count)

    def named(lengths, offset_by):
        used = int((lengths > 0).sum())
        fixed = max(1, used // 4)
        passed = fixed + (places - fixed + offset_by * (used - fixed)) % max(1, count - fixed)
        return jnp.zeros((count,), jnp.int32).at[order[jnp.where(places < fixed, places, passed)]].set(jnp.asarray(lengths, jnp.int32))

    lengths = jnp.where(number % 4 == 0, named(heavy_load, number // 4), named(ordinary, number - number // 4 - 1))
    mixed = jax.random.permutation(jax.random.fold_in(own, 3), count)
    donor, receiver = mixed[0:count // 2 * 2:2], mixed[1:count // 2 * 2:2]
    slack = jnp.minimum(lengths[donor] - 1, limit - lengths[receiver]) // 2
    slack = jnp.where((donor == order[0]) | (receiver == order[0]) | (lengths[receiver] == 0), 0, jnp.maximum(slack, 0))
    passed = jax.random.randint(jax.random.fold_in(own, 4), (count // 2,), 0, 1 << 20) % (slack + 1)
    lengths = lengths.at[donor].add(-passed).at[receiver].add(passed)
    items = jnp.searchsorted(jnp.cumsum(lengths), jnp.arange(rows * top), side="right").astype(jnp.int32)
    grid = items.reshape(top, rows).T
    grid = grid[jax.random.permutation(jax.random.fold_in(own, 1), rows)]
    offset_by = jax.random.randint(jax.random.fold_in(own, 2), (rows, 1), 0, top)
    return jnp.take_along_axis(grid, (jnp.arange(top)[None, :] + offset_by) % top, axis=1)


def shares(count, total, limit, slope, full):
    loads = [(1 << 20) // math.isqrt(grade ** slope) + 1 for grade in range(1, count + 1)]
    largest = limit if full else min(limit, max(-(-total // count), total * loads[0] // sum(loads)))
    least = 1 if total - largest >= count - 1 else 0
    given, spare = [largest] + [least] * (count - 1), total - largest - least * (count - 1)
    while spare > 0:
        free = [i for i in range(1, count) if given[i] < largest] or [i for i in range(1, count) if given[i] < limit]
        pool, budget = sum([loads[i] for i in free]), spare
        for i in free:
            addition = min(limit - given[i], max(1, budget * loads[i] // pool), spare)
            given[i] = given[i] + addition
            spare = spare - addition
    return np.array(given)


def scatter_about(rng, shape, scale, most, pieces=(), held_as=jnp.bfloat16):
    drawn = scale * jax.random.normal(rng, shape, jnp.float32)
    if pieces:
        drawn = drawn * steps_of(rng, shape, pieces, -0.22, 0.18)
    return jnp.clip(drawn, -most, most).astype(held_as)


def setup_inputs(seed: int = 0) -> dict:
    splits = jax.random.split(jax.random.key(seed), 8)
    tokens = scatter_about(splits[0], (TOKENS, D), 1.0, 6.0, ((0, 32),))
    out_grad = scatter_about(splits[1], (TOKENS, D), 1.0, 6.0, ((0, 32),))
    expert_ids_keys = jax.random.split(jax.random.fold_in(splits[2], 1), TOKENS // TOK_DEV)
    expert_ids_turns = jax.random.permutation(jax.random.fold_in(splits[2], 3), TOKENS // TOK_DEV)
    expert_ids = jax.vmap(lambda own, number: routed_block(jax.random.fold_in(splits[2], 2), own, number, TOK_DEV, EXPERTS, TOP, CAP, 2))(expert_ids_keys, expert_ids_turns).reshape((TOKENS, TOP))
    gate_values = jnp.clip(0.05 + 0.95 * jax.random.uniform(splits[3], (TOKENS, TOP), jnp.float32) ** steps_of(splits[3], (TOKENS, TOP), ((0, 32),), -0.2, 0.2), 0.05, 1.0)
    w_gate = scatter_about(splits[4], (EXPERTS, D, FF), D ** -0.5, 0.125, ((0, 16), (2, 2)))
    w_up = scatter_about(splits[5], (EXPERTS, D, FF), D ** -0.5, 0.125, ((0, 16), (2, 2)))
    w_down = scatter_about(splits[6], (EXPERTS, FF, D), FF ** -0.5, 0.1875, ((0, 16), (1, 2)))
    return {"tokens": tokens, "out_grad": out_grad, "expert_ids": expert_ids, "gate_values": gate_values, "w_gate": w_gate, "w_up": w_up, "w_down": w_down}


def reference(tokens, out_grad, expert_ids, gate_values, w_gate, w_up, w_down):
    blocks = TOKENS // TOK_DEV
    id_blocks = expert_ids.reshape(blocks, TOK_DEV * TOP)
    onehot = (id_blocks[:, :, None] == jnp.arange(EXPERTS, dtype=jnp.int32)[None, None, :]).astype(jnp.int32)
    before = jnp.cumsum(onehot, axis=1) - onehot
    slot_rank = jnp.sum(before * onehot, axis=2).astype(jnp.int32)
    block_index = jnp.arange(blocks, dtype=jnp.int32)[:, None]
    batch_index = block_index // N_EXPERT
    source_index = block_index % N_EXPERT
    position = id_blocks * ROWS + (batch_index * N_EXPERT + source_index) * CAP + slot_rank
    token_index = block_index * TOK_DEV + (jnp.arange(TOK_DEV * TOP, dtype=jnp.int32) // TOP)[None, :]
    token_index = jnp.broadcast_to(token_index, position.shape).astype(jnp.int32)
    table = jnp.full((EXPERTS * ROWS,), TOKENS, dtype=jnp.int32)
    table = table.at[position.reshape(-1)].set(token_index.reshape(-1)).reshape(EXPERTS, ROWS)
    gate_table = jnp.zeros((EXPERTS * ROWS,), dtype=jnp.float32)
    gate_table = gate_table.at[position.reshape(-1)].set(gate_values.reshape(-1)).reshape(EXPERTS, ROWS)
    tokens_pad = jnp.concatenate([tokens, jnp.zeros((1, D), dtype=tokens.dtype)], axis=0)
    grads_pad = jnp.concatenate([out_grad, jnp.zeros((1, D), dtype=out_grad.dtype)], axis=0)
    block_width = FF // N_DP

    def one_expert(operands):
        index_row, gate_row, weight_gate, weight_up, weight_down = operands
        x_rows = tokens_pad[index_row]
        g_rows = (gate_row[:, None] * grads_pad[index_row].astype(jnp.float32)).astype(jnp.bfloat16)
        gate_pre = jnp.dot(x_rows, weight_gate, preferred_element_type=jnp.float32)
        up_pre = jnp.dot(x_rows, weight_up, preferred_element_type=jnp.float32)
        sigmoid_val = jax.nn.sigmoid(gate_pre)
        silu_val = gate_pre * sigmoid_val
        activation = (silu_val * up_pre).astype(jnp.bfloat16)
        act_grad = jnp.dot(g_rows, weight_down.T, preferred_element_type=jnp.float32)
        up_grad = (act_grad * silu_val).astype(jnp.bfloat16)
        gate_grad = (act_grad * up_pre * sigmoid_val * (1.0 + gate_pre * (1.0 - sigmoid_val))).astype(jnp.bfloat16)
        grad_g = jnp.dot(x_rows.T, gate_grad, preferred_element_type=jnp.float32)
        grad_u = jnp.dot(x_rows.T, up_grad, preferred_element_type=jnp.float32)
        grad_d = jnp.dot(activation.T, g_rows, preferred_element_type=jnp.float32)
        row_sums = jnp.zeros((ROWS, D), dtype=jnp.float32)
        for block in range(N_DP):
            low = block * block_width
            high = low + block_width
            term = jnp.dot(gate_grad[:, low:high], weight_gate[:, low:high].T, preferred_element_type=jnp.float32)
            term = term + jnp.dot(up_grad[:, low:high], weight_up[:, low:high].T, preferred_element_type=jnp.float32)
            rounded = lax.optimization_barrier(term.astype(jnp.bfloat16))
            row_sums = row_sums + rounded.astype(jnp.float32)
        return grad_g, grad_u, grad_d, row_sums

    grad_gate, grad_up, grad_down, row_grads = lax.map(one_expert, (table, gate_table, w_gate, w_up, w_down))
    summed = jnp.zeros((TOKENS + 1, D), dtype=jnp.float32)
    summed = summed.at[table.reshape(-1)].add(row_grads.reshape(EXPERTS * ROWS, D))
    grad_tokens = summed[:TOKENS].astype(jnp.bfloat16)
    return grad_tokens, grad_gate, grad_up, grad_down
```

```python
import jax
import jax.numpy as jnp
from jax import lax
from jax.sharding import PartitionSpec as P

AXES = ("dp", "expert")


def contract_last(left_op, right_op):
    return lax.dot_general(
        left_op, right_op, (((1,), (1,)), ((), ())), preferred_element_type=jnp.float32
    )


def contract_first(left_op, right_op):
    return lax.dot_general(
        left_op, right_op, (((0,), (0,)), ((), ())), preferred_element_type=jnp.float32
    )


def contract_inner(left_op, right_op):
    return jnp.dot(left_op, right_op, preferred_element_type=jnp.float32)


def hidden_grads(gate_pre, up_pre, act_grad):
    sigmoid_val = jax.nn.sigmoid(gate_pre)
    silu_val = gate_pre * sigmoid_val
    activation = (silu_val * up_pre).astype(jnp.bfloat16)
    up_grad = (act_grad * silu_val).astype(jnp.bfloat16)
    gate_grad = (act_grad * up_pre * sigmoid_val * (1.0 + gate_pre * (1.0 - sigmoid_val))).astype(
        jnp.bfloat16
    )
    return activation, gate_grad, up_grad


def exchange_stages(device_count):
    top = device_count // 2
    far = [bit for bit in (1 << i for i in range(2, 32)) if bit < top]
    masks = [0]
    for bit in far:
        masks = masks + [mask | bit for mask in masks]
    return [[(mask, mask) for mask in masks[1:]], [(2, top)], [(top, 2)], [(1, 1)]]


def swap(value, masks, device_count):
    even, odd = masks
    pairs = [(i, i ^ (odd if i % 2 else even)) for i in range(device_count)]
    return lax.ppermute(value, AXES, pairs)


def gate_columns(expert_ids, gate_values, expert_count, width):
    named = expert_ids[:, :, None] == jnp.arange(expert_count, dtype=jnp.int32)[None, None, :]
    weight = jnp.sum(jnp.where(named, gate_values[:, :, None], 0.0), axis=1)
    high = lax.reduce_precision(weight, 8, 7)
    middle = lax.reduce_precision(weight - high, 8, 7)
    low = weight - high - middle
    pieces = jnp.concatenate([high, middle, low], axis=1)
    return jnp.pad(pieces, ((0, 0), (0, width - pieces.shape[1]))).astype(jnp.bfloat16)


def all_rows(tokens, out_grad, expert_ids, gate_values, w_gate, w_up, w_down):
    expert_count = lax.axis_size("expert")
    device_count = lax.axis_size("dp") * expert_count
    model_width = tokens.shape[1]
    gate_width = -(-3 * expert_count // 128) * 128
    stages = exchange_stages(device_count)
    rows = jnp.concatenate(
        [tokens, out_grad, gate_columns(expert_ids, gate_values, expert_count, gate_width)], axis=1
    )
    for stage in stages:
        rows = jnp.concatenate([rows] + [swap(rows, mask, device_count) for mask in stage], axis=0)
    x_rows = rows[:, :model_width]
    pieces = rows[:, 2 * model_width :].astype(jnp.float32)
    column = jnp.arange(gate_width, dtype=jnp.int32)[None, :]
    mine = (column % expert_count == lax.axis_index("expert")) & (column < 3 * expert_count)
    gate = jnp.sum(jnp.where(mine, pieces, 0.0), axis=1, keepdims=True)
    g_rows = (gate * rows[:, model_width : 2 * model_width].astype(jnp.float32)).astype(
        jnp.bfloat16
    )
    activation, gate_grad, up_grad = hidden_grads(
        contract_inner(x_rows, w_gate[0]),
        contract_inner(x_rows, w_up[0]),
        contract_last(g_rows, w_down[0]),
    )
    sums = contract_last(gate_grad, w_gate[0]) + contract_last(up_grad, w_up[0])
    sums = sums.astype(jnp.bfloat16)
    for stage in reversed(stages):
        parts = jnp.split(sums, len(stage) + 1, axis=0)
        total = parts[0].astype(jnp.float32)
        for part, mask in zip(parts[1:], stage):
            total = total + swap(part, mask, device_count).astype(jnp.float32)
        sums = total.astype(jnp.bfloat16)
    grad_gate = contract_first(x_rows, gate_grad)
    grad_up = contract_first(x_rows, up_grad)
    grad_down = contract_first(activation, g_rows)
    return sums, grad_gate[None], grad_up[None], grad_down[None]


def slot_table(expert_ids, gate_values, expert_count, capacity):
    tok_rows, top_count = expert_ids.shape
    flat_ids = expert_ids.reshape(-1)
    onehot = (flat_ids[:, None] == jnp.arange(expert_count, dtype=jnp.int32)[None, :]).astype(
        jnp.int32
    )
    before = jnp.cumsum(onehot, axis=0) - onehot
    slot_rank = jnp.sum(before * onehot, axis=1)
    slot_index = flat_ids * capacity + slot_rank
    slot_hits = (
        slot_index[:, None] == jnp.arange(expert_count * capacity, dtype=jnp.int32)[None, :]
    ).astype(jnp.float32)
    owner_row = jnp.arange(tok_rows * top_count, dtype=jnp.int32) // top_count
    token_hits = (owner_row[:, None] == jnp.arange(tok_rows, dtype=jnp.int32)[None, :]).astype(
        jnp.float32
    )
    weighted = slot_hits * gate_values.reshape(-1)[:, None]
    return jnp.dot(weighted.T, token_hits, precision=lax.Precision.HIGHEST)


def slot_rows(tokens, out_grad, expert_ids, gate_values, w_gate, w_up, w_down):
    expert_count = lax.axis_size("expert")
    tok_rows, model_width = tokens.shape
    capacity = slots_of(expert_ids.shape, expert_count)
    slot_count = expert_count * capacity
    gate_table = slot_table(expert_ids, gate_values, expert_count, capacity)
    pick_table = (gate_table > 0.0).astype(jnp.float32)

    def to_experts(rows):
        return lax.all_to_all(
            rows.reshape(expert_count, capacity, model_width),
            "expert",
            split_axis=0,
            concat_axis=0,
            tiled=True,
        ).reshape(slot_count, model_width)

    sent_rows = contract_inner(pick_table.astype(jnp.bfloat16), tokens).astype(jnp.bfloat16)
    sent_grads = jnp.dot(
        gate_table, out_grad.astype(jnp.float32), precision=lax.Precision.HIGHEST
    ).astype(jnp.bfloat16)
    x_rows = lax.all_gather(to_experts(sent_rows), "dp", axis=0, tiled=True)
    g_rows = lax.all_gather(to_experts(sent_grads), "dp", axis=0, tiled=True)
    activation, gate_grad, up_grad = hidden_grads(
        contract_inner(x_rows, w_gate[0]),
        contract_inner(x_rows, w_up[0]),
        contract_last(g_rows, w_down[0]),
    )
    sums = contract_last(gate_grad, w_gate[0]) + contract_last(up_grad, w_up[0])
    own_sums = lax.psum_scatter(
        sums.astype(jnp.bfloat16), "dp", scatter_dimension=0, tiled=True
    )
    back_rows = to_experts(own_sums).astype(jnp.float32)
    token_grad = jnp.dot(pick_table.T, back_rows, precision=lax.Precision.HIGHEST)
    grad_gate = contract_first(x_rows, gate_grad)
    grad_up = contract_first(x_rows, up_grad)
    grad_down = contract_first(activation, g_rows)
    return token_grad.astype(jnp.bfloat16), grad_gate[None], grad_up[None], grad_down[None]


def slots_of(ids_shape, expert_count):
    return 2 * ids_shape[0] * ids_shape[1] // expert_count


def solution(mesh):
    dp_count, expert_count = mesh.shape["dp"], mesh.shape["expert"]
    device_count = dp_count * expert_count

    def shards(tokens, out_grad, expert_ids, gate_values, w_gate, w_up, w_down):
        capacity = slots_of(expert_ids.shape, expert_count)
        paired = device_count >= 8 and device_count & (device_count - 1) == 0
        every_row = paired and expert_count * capacity >= expert_count * tokens.shape[0]
        body = all_rows if every_row else slot_rows
        return body(tokens, out_grad, expert_ids, gate_values, w_gate, w_up, w_down)

    split = P(AXES, None)
    return jax.shard_map(
        shards,
        mesh=mesh,
        in_specs=(split, split, split, split)
        + (P("expert", None, "dp"), P("expert", None, "dp"), P("expert", "dp", None)),
        out_specs=(split, P("expert", None, "dp"), P("expert", None, "dp"), P("expert", "dp", None)),
        check_vma=False,
    )
```

```python
import functools

import jax
import jax.numpy as jnp
from jax import lax
from jax.experimental import pallas as pl
from jax.experimental.pallas import tpu as pltpu
from jax.sharding import PartitionSpec as P


AXES = ("dp", "expert")


def contract_last(left_op, right_op):
    return lax.dot_general(
        left_op, right_op, (((1,), (1,)), ((), ())), preferred_element_type=jnp.float32
    )


def contract_first(left_op, right_op):
    return lax.dot_general(
        left_op, right_op, (((0,), (0,)), ((), ())), preferred_element_type=jnp.float32
    )


def contract_inner(left_op, right_op):
    return jnp.dot(left_op, right_op, preferred_element_type=jnp.float32)


def hidden_grads(gate_pre, up_pre, act_grad):
    sigmoid_val = jax.nn.sigmoid(gate_pre)
    silu_val = gate_pre * sigmoid_val
    activation = (silu_val * up_pre).astype(jnp.bfloat16)
    up_grad = (act_grad * silu_val).astype(jnp.bfloat16)
    gate_grad = (act_grad * up_pre * sigmoid_val * (1.0 + gate_pre * (1.0 - sigmoid_val))).astype(
        jnp.bfloat16
    )
    return activation, gate_grad, up_grad


def swap(value, masks, device_count):
    even, odd = masks
    pairs = [(i, i ^ (odd if i % 2 else even)) for i in range(device_count)]
    return lax.ppermute(value, AXES, pairs)


def row_kernel(expert_count, tokens, out_grad, expert_ids, gate_values, rows, ids_held,
               values_held, copied):
    model_width = tokens.shape[1]
    gate_width = rows.shape[1] - 2 * model_width
    moves = (
        (expert_ids, ids_held),
        (gate_values, values_held),
        (tokens, rows.at[:, pl.ds(0, model_width)]),
        (out_grad, rows.at[:, pl.ds(model_width, model_width)]),
    )
    copies = [
        pltpu.make_async_copy(source, target, copied.at[i])
        for i, (source, target) in enumerate(moves)
    ]
    for copy in copies:
        copy.start()
    copies[0].wait()
    copies[1].wait()
    column = lax.broadcasted_iota(jnp.int32, (tokens.shape[0], gate_width), 1)
    expert = lax.rem(column, expert_count)
    ids, values = ids_held[...], values_held[...]
    weight = jnp.zeros(column.shape, jnp.float32)
    for k in range(ids.shape[1]):
        weight = weight + jnp.where(ids[:, k : k + 1] == expert, values[:, k : k + 1], 0.0)
    high = weight.astype(jnp.bfloat16).astype(jnp.float32)
    middle = (weight - high).astype(jnp.bfloat16).astype(jnp.float32)
    low = weight - high - middle
    place = lax.div(column, expert_count)
    piece = jnp.where(place == 0, high, jnp.where(place == 1, middle, low))
    piece = jnp.where(place < 3, piece, 0.0)
    rows[:, 2 * model_width :] = piece.astype(jnp.bfloat16)
    copies[2].wait()
    copies[3].wait()


def in_hbm(*values):
    return [pltpu.with_memory_space_constraint(value, pltpu.HBM) for value in values]


def routed_rows(tokens, out_grad, expert_ids, gate_values, expert_count):
    gate_width = -(-3 * expert_count // 128) * 128
    return pl.pallas_call(
        functools.partial(row_kernel, expert_count),
        out_shape=jax.ShapeDtypeStruct(
            (tokens.shape[0], 2 * tokens.shape[1] + gate_width), jnp.bfloat16
        ),
        in_specs=[pl.BlockSpec(memory_space=pltpu.HBM)] * 4,
        out_specs=pl.BlockSpec(memory_space=pltpu.VMEM),
        scratch_shapes=[
            pltpu.VMEM(expert_ids.shape, expert_ids.dtype),
            pltpu.VMEM(gate_values.shape, gate_values.dtype),
            pltpu.SemaphoreType.DMA((4,)),
        ],
        compiler_params=pltpu.CompilerParams(vmem_limit_bytes=4 << 20),
        name="routed_rows",
    )(*in_hbm(tokens, out_grad, expert_ids, gate_values))


def bring_kernel(count, *refs):
    sources, targets, copied = refs[:count], refs[count:-1], refs[-1]
    copies = [
        pltpu.make_async_copy(source, target, copied.at[i])
        for i, (source, target) in enumerate(zip(sources, targets))
    ]
    for copy in copies:
        copy.start()
    for copy in copies:
        copy.wait()


def bring(values):
    return pl.pallas_call(
        functools.partial(bring_kernel, len(values)),
        out_shape=[jax.ShapeDtypeStruct(value.shape, value.dtype) for value in values],
        in_specs=[pl.BlockSpec(memory_space=pltpu.HBM)] * len(values),
        out_specs=[pl.BlockSpec(memory_space=pltpu.VMEM)] * len(values),
        scratch_shapes=[pltpu.SemaphoreType.DMA((len(values),))],
        compiler_params=pltpu.CompilerParams(vmem_limit_bytes=8 << 20),
        name="bring",
    )(*in_hbm(*values))


def pass_kernel(expert_count, own_1, own_2, sib_1, sib_2, w_gate, w_up, w_down, *outs):
    activation, gate_grad, up_grad, g_rows, own_sums, sib_sums = outs
    model_width = w_gate.shape[0]
    half = own_1.shape[0]
    gate_width = own_1.shape[1] - 2 * model_width
    column = lax.broadcasted_iota(jnp.int32, (1, gate_width), 1)
    mine = (column < 3 * expert_count) & (
        lax.rem(column, expert_count) == lax.axis_index("expert")
    )
    for i, piece in enumerate((own_1, own_2, sib_1, sib_2)):
        pieces = piece[:, 2 * model_width :].astype(jnp.float32)
        gate = jnp.sum(jnp.where(mine, pieces, 0.0), axis=1, keepdims=True)
        grads = gate * piece[:, model_width : 2 * model_width].astype(jnp.float32)
        g_rows[i * half : (i + 1) * half, :] = grads.astype(jnp.bfloat16)
    x_rows = jnp.concatenate(
        [piece[:, :model_width] for piece in (own_1, own_2, sib_1, sib_2)], axis=0
    )
    act_value, gate_value, up_value = hidden_grads(
        contract_inner(x_rows, w_gate[...]),
        contract_inner(x_rows, w_up[...]),
        contract_last(g_rows[...], w_down[...]),
    )
    activation[...] = act_value
    gate_grad[...] = gate_value
    up_grad[...] = up_value
    sums = contract_last(gate_value, w_gate[...]) + contract_last(up_value, w_up[...])
    sums = sums.astype(jnp.bfloat16)
    quarter = half // 2
    for to, at in enumerate((0, 2, 1, 3)):
        own_sums[to * quarter : (to + 1) * quarter, :] = sums[at * quarter : (at + 1) * quarter]
        at = at + 4
        sib_sums[to * quarter : (to + 1) * quarter, :] = sums[at * quarter : (at + 1) * quarter]


def expert_pass(pieces, weights, expert_count):
    rows = 4 * pieces[0].shape[0]
    model_width, hidden_units = weights[0].shape
    hidden = jax.ShapeDtypeStruct((rows, hidden_units), jnp.bfloat16)
    wide = jax.ShapeDtypeStruct((rows, model_width), jnp.bfloat16)
    part = jax.ShapeDtypeStruct((rows // 2, model_width), jnp.bfloat16)
    in_vmem = pl.BlockSpec(memory_space=pltpu.VMEM)
    return pl.pallas_call(
        functools.partial(pass_kernel, expert_count),
        out_shape=(hidden, hidden, hidden, wide, part, part),
        in_specs=[in_vmem] * 7,
        out_specs=(in_vmem,) * 6,
        cost_estimate=pl.CostEstimate(
            flops=10 * rows * model_width * hidden_units,
            bytes_accessed=6 * model_width * hidden_units,
            transcendentals=rows * hidden_units,
        ),
        compiler_params=pltpu.CompilerParams(vmem_limit_bytes=24 << 20),
    )(*pieces, *weights)


def outer_kernel(left_count, right_count, steps, *refs):
    lefts, refs = refs[:left_count], refs[left_count:]
    each = (len(refs) - 2 * right_count - 1) // right_count
    rights, refs = refs[: each * right_count], refs[each * right_count :]
    outs, held, copied = refs[:right_count], refs[right_count:-1], refs[-1]
    width = outs[0].shape[0] // steps
    copies = []
    for step in range(steps):
        block = pl.ds(step * width, width)
        left = jnp.concatenate([value[:, block] for value in lefts], axis=0)
        for i in range(right_count):
            right = [value[...] for value in rights[i * each : (i + 1) * each]]
            held[i][block, :] = contract_first(left, jnp.concatenate(right, axis=0))
            copies.append(
                pltpu.make_async_copy(
                    held[i].at[block, :], outs[i].at[block, :], copied.at[len(copies)]
                )
            )
            copies[-1].start()
    for copy in copies:
        copy.wait()


def outer_sums(lefts, left_width, rights, steps):
    rows = sum(value.shape[0] for value in lefts)
    right_width = rights[0][0].shape[1]
    shape = (left_width, right_width)
    values = list(lefts) + [value for right in rights for value in right]
    return pl.pallas_call(
        functools.partial(outer_kernel, len(lefts), len(rights), steps),
        out_shape=[jax.ShapeDtypeStruct(shape, jnp.float32)] * len(rights),
        in_specs=[pl.BlockSpec(memory_space=pltpu.VMEM)] * len(values),
        out_specs=[pl.BlockSpec(memory_space=pltpu.HBM)] * len(rights),
        scratch_shapes=[pltpu.VMEM(shape, jnp.float32)] * len(rights)
        + [pltpu.SemaphoreType.DMA((steps * len(rights),))],
        cost_estimate=pl.CostEstimate(
            flops=2 * rows * left_width * right_width * len(rights),
            bytes_accessed=4 * left_width * right_width * len(rights),
            transcendentals=0,
        ),
        compiler_params=pltpu.CompilerParams(vmem_limit_bytes=24 << 20),
    )(*values)


def total(*values):
    return sum(value.astype(jnp.float32) for value in values).astype(jnp.bfloat16)


def add(left, right):
    return total(left, right)


def all_rows(tokens, out_grad, expert_ids, gate_values, w_gate, w_up, w_down):
    expert_count = lax.axis_size("expert")
    device_count = lax.axis_size("dp") * expert_count
    model_width, hidden_units = w_gate.shape[1:]
    top = device_count // 2
    side, cross, core = (2, top), (top, 2), (1, 1)
    both = (2 + top, 2 + top)
    line = top // 4

    def go(value, masks):
        return swap(value, masks, device_count)

    def along(value, step):
        return go(value, (4 * step, 4 * step))

    rows = routed_rows(tokens, out_grad, expert_ids, gate_values, expert_count)
    lines = [rows] + [along(rows, i) for i in range(1, line)]
    weights = bring((w_gate[0], w_up[0], w_down[0]))
    middle = line // 2
    early, early_sib, late = [], [], []
    for part in (lines[:middle], lines[middle:]):
        part = jnp.concatenate(part, axis=0)
        part = jnp.concatenate([part, go(part, side)], axis=0)
        early.append(part)
        late.append(go(part, cross))
        early_sib.append(go(part, core))
    early_out = expert_pass(early + early_sib, weights, expert_count)
    late, _ = lax.optimization_barrier((late, early_out[0]))
    late_sib = [go(part, core) for part in late]
    late_out = expert_pass(late + late_sib, weights, expert_count)
    half = early_out[4].shape[0] // 2
    early_sums = add(early_out[4], go(early_out[5], core))
    sided = go(early_sums[half:], side)
    late_sums = add(late_out[4], go(late_out[5], core))
    crossed = go(late_sums[:half], cross)
    returned = go(late_sums[half:], both)
    acts, gates, ups, g_rows = zip(early_out[:4], late_out[:4])
    pieces = early + early_sib + late + late_sib
    grad_gate, grad_up = outer_sums(pieces, model_width, (gates, ups), 8)
    crossed, grad_gate, grad_up = lax.optimization_barrier((crossed, grad_gate, grad_up))
    sums = total(early_sums[:half], sided, crossed, returned)
    parts = jnp.split(sums, line, axis=0)
    back = [along(parts[i], i) for i in range(1, line)]
    (grad_down,) = outer_sums(acts, hidden_units, (g_rows,), 4)
    return total(parts[0], *back), grad_gate[None], grad_up[None], grad_down[None]


def slot_table(expert_ids, gate_values, expert_count, capacity):
    tok_rows, top_count = expert_ids.shape
    flat_ids = expert_ids.reshape(-1)
    onehot = (flat_ids[:, None] == jnp.arange(expert_count, dtype=jnp.int32)[None, :]).astype(
        jnp.int32
    )
    before = jnp.cumsum(onehot, axis=0) - onehot
    slot_rank = jnp.sum(before * onehot, axis=1)
    slot_index = flat_ids * capacity + slot_rank
    slot_hits = (
        slot_index[:, None] == jnp.arange(expert_count * capacity, dtype=jnp.int32)[None, :]
    ).astype(jnp.float32)
    owner_row = jnp.arange(tok_rows * top_count, dtype=jnp.int32) // top_count
    token_hits = (owner_row[:, None] == jnp.arange(tok_rows, dtype=jnp.int32)[None, :]).astype(
        jnp.float32
    )
    weighted = slot_hits * gate_values.reshape(-1)[:, None]
    return jnp.dot(weighted.T, token_hits, precision=lax.Precision.HIGHEST)


def slot_rows(tokens, out_grad, expert_ids, gate_values, w_gate, w_up, w_down):
    expert_count = lax.axis_size("expert")
    _, model_width = tokens.shape
    capacity = slots_of(expert_ids.shape, expert_count)
    slot_count = expert_count * capacity
    gate_table = slot_table(expert_ids, gate_values, expert_count, capacity)
    pick_table = (gate_table > 0.0).astype(jnp.float32)

    def to_experts(rows):
        return lax.all_to_all(
            rows.reshape(expert_count, capacity, model_width),
            "expert",
            split_axis=0,
            concat_axis=0,
            tiled=True,
        ).reshape(slot_count, model_width)

    sent_rows = contract_inner(pick_table.astype(jnp.bfloat16), tokens).astype(jnp.bfloat16)
    sent_grads = jnp.dot(
        gate_table, out_grad.astype(jnp.float32), precision=lax.Precision.HIGHEST
    ).astype(jnp.bfloat16)
    x_rows = lax.all_gather(to_experts(sent_rows), "dp", axis=0, tiled=True)
    g_rows = lax.all_gather(to_experts(sent_grads), "dp", axis=0, tiled=True)
    activation, gate_grad, up_grad = hidden_grads(
        contract_inner(x_rows, w_gate[0]),
        contract_inner(x_rows, w_up[0]),
        contract_last(g_rows, w_down[0]),
    )
    sums = contract_last(gate_grad, w_gate[0]) + contract_last(up_grad, w_up[0])
    own_sums = lax.psum_scatter(
        sums.astype(jnp.bfloat16), "dp", scatter_dimension=0, tiled=True
    )
    back_rows = to_experts(own_sums).astype(jnp.float32)
    token_grad = jnp.dot(pick_table.T, back_rows, precision=lax.Precision.HIGHEST)
    grad_gate = contract_first(x_rows, gate_grad)
    grad_up = contract_first(x_rows, up_grad)
    grad_down = contract_first(activation, g_rows)
    return token_grad.astype(jnp.bfloat16), grad_gate[None], grad_up[None], grad_down[None]


def slots_of(ids_shape, expert_count):
    return 2 * ids_shape[0] * ids_shape[1] // expert_count


def solution(mesh):
    dp_count, expert_count = mesh.shape["dp"], mesh.shape["expert"]
    device_count = dp_count * expert_count

    def shards(tokens, out_grad, expert_ids, gate_values, w_gate, w_up, w_down):
        capacity = slots_of(expert_ids.shape, expert_count)
        paired = device_count >= 8 and device_count & (device_count - 1) == 0
        every_row = paired and expert_count * capacity >= expert_count * tokens.shape[0]
        body = all_rows if every_row else slot_rows
        return body(tokens, out_grad, expert_ids, gate_values, w_gate, w_up, w_down)

    split = P(AXES, None)
    return jax.shard_map(
        shards,
        mesh=mesh,
        in_specs=(split, split, split, split)
        + (P("expert", None, "dp"), P("expert", None, "dp"), P("expert", "dp", None)),
        out_specs=(split, P("expert", None, "dp"), P("expert", None, "dp"), P("expert", "dp", None)),
        check_vma=False,
    )
```

```python
import functools

import jax
import jax.numpy as jnp
from jax import lax
from jax.experimental import pallas as pl
from jax.experimental.pallas import tpu as pltpu
from jax.sharding import PartitionSpec as P


AXES = ("dp", "expert")


def contract_last(left_op, right_op):
    return lax.dot_general(
        left_op, right_op, (((1,), (1,)), ((), ())), preferred_element_type=jnp.float32
    )


def contract_first(left_op, right_op):
    return lax.dot_general(
        left_op, right_op, (((0,), (0,)), ((), ())), preferred_element_type=jnp.float32
    )


def contract_inner(left_op, right_op):
    return jnp.dot(left_op, right_op, preferred_element_type=jnp.float32)


def hidden_grads(gate_pre, up_pre, act_grad):
    sigmoid_val = jax.nn.sigmoid(gate_pre)
    silu_val = gate_pre * sigmoid_val
    activation = (silu_val * up_pre).astype(jnp.bfloat16)
    up_grad = (act_grad * silu_val).astype(jnp.bfloat16)
    gate_grad = (act_grad * up_pre * sigmoid_val * (1.0 + gate_pre * (1.0 - sigmoid_val))).astype(
        jnp.bfloat16
    )
    return activation, gate_grad, up_grad


def swap(value, masks, device_count):
    even, odd = masks
    pairs = [(i, i ^ (odd if i % 2 else even)) for i in range(device_count)]
    return lax.ppermute(value, AXES, pairs)


def row_kernel(expert_count, tokens, out_grad, expert_ids, gate_values, rows, ids_held,
               values_held, copied):
    model_width = tokens.shape[1]
    gate_width = rows.shape[1] - 2 * model_width
    moves = (
        (expert_ids, ids_held),
        (gate_values, values_held),
        (tokens, rows.at[:, pl.ds(0, model_width)]),
        (out_grad, rows.at[:, pl.ds(model_width, model_width)]),
    )
    copies = [
        pltpu.make_async_copy(source, target, copied.at[i])
        for i, (source, target) in enumerate(moves)
    ]
    for copy in copies:
        copy.start()
    copies[0].wait()
    copies[1].wait()
    column = lax.broadcasted_iota(jnp.int32, (tokens.shape[0], gate_width), 1)
    expert = lax.rem(column, expert_count)
    ids, values = ids_held[...], values_held[...]
    weight = jnp.zeros(column.shape, jnp.float32)
    for k in range(ids.shape[1]):
        weight = weight + jnp.where(ids[:, k : k + 1] == expert, values[:, k : k + 1], 0.0)
    high = weight.astype(jnp.bfloat16).astype(jnp.float32)
    middle = (weight - high).astype(jnp.bfloat16).astype(jnp.float32)
    low = weight - high - middle
    place = lax.div(column, expert_count)
    piece = jnp.where(place == 0, high, jnp.where(place == 1, middle, low))
    piece = jnp.where(place < 3, piece, 0.0)
    rows[:, 2 * model_width :] = piece.astype(jnp.bfloat16)
    copies[2].wait()
    copies[3].wait()


def in_hbm(*values):
    return [pltpu.with_memory_space_constraint(value, pltpu.HBM) for value in values]


def routed_rows(tokens, out_grad, expert_ids, gate_values, expert_count):
    gate_width = -(-3 * expert_count // 128) * 128
    return pl.pallas_call(
        functools.partial(row_kernel, expert_count),
        out_shape=jax.ShapeDtypeStruct(
            (tokens.shape[0], 2 * tokens.shape[1] + gate_width), jnp.bfloat16
        ),
        in_specs=[pl.BlockSpec(memory_space=pltpu.HBM)] * 4,
        out_specs=pl.BlockSpec(memory_space=pltpu.VMEM),
        scratch_shapes=[
            pltpu.VMEM(expert_ids.shape, expert_ids.dtype),
            pltpu.VMEM(gate_values.shape, gate_values.dtype),
            pltpu.SemaphoreType.DMA((4,)),
        ],
        compiler_params=pltpu.CompilerParams(vmem_limit_bytes=4 << 20),
        name="routed_rows",
    )(*in_hbm(tokens, out_grad, expert_ids, gate_values))


def bring_kernel(count, *refs):
    sources, targets, copied = refs[:count], refs[count:-1], refs[-1]
    copies = [
        pltpu.make_async_copy(source, target, copied.at[i])
        for i, (source, target) in enumerate(zip(sources, targets))
    ]
    for copy in copies:
        copy.start()
    for copy in copies:
        copy.wait()


def column_kernel(expert_count, mine):
    column = lax.broadcasted_iota(jnp.int32, mine.shape, 1)
    own = lax.rem(column, expert_count) == lax.axis_index("expert")
    mine[...] = jnp.where(own & (column < 3 * expert_count), 1.0, 0.0)


def own_columns(expert_count, gate_width):
    return pl.pallas_call(
        functools.partial(column_kernel, expert_count),
        out_shape=jax.ShapeDtypeStruct((1, gate_width), jnp.float32),
        out_specs=pl.BlockSpec(memory_space=pltpu.VMEM),
        compiler_params=pltpu.CompilerParams(vmem_limit_bytes=1 << 20),
        name="own_columns",
    )()


def bring(values):
    return pl.pallas_call(
        functools.partial(bring_kernel, len(values)),
        out_shape=[jax.ShapeDtypeStruct(value.shape, value.dtype) for value in values],
        in_specs=[pl.BlockSpec(memory_space=pltpu.HBM)] * len(values),
        out_specs=[pl.BlockSpec(memory_space=pltpu.VMEM)] * len(values),
        scratch_shapes=[pltpu.SemaphoreType.DMA((len(values),))],
        compiler_params=pltpu.CompilerParams(vmem_limit_bytes=8 << 20),
        name="bring",
    )(*in_hbm(*values))


def pass_kernel(piece_count, *refs):
    pieces, (w_gate, w_up, w_down, mine), outs = (
        refs[:piece_count],
        refs[piece_count : piece_count + 4],
        refs[piece_count + 4 :],
    )
    activation, gate_grad, up_grad, g_rows, own_sums, sib_sums = outs
    model_width = w_gate.shape[0]
    row = 0
    for piece in pieces:
        weights = piece[:, 2 * model_width :].astype(jnp.float32)
        gate = jnp.sum(weights * mine[...], axis=1, keepdims=True)
        grads = gate * piece[:, model_width : 2 * model_width].astype(jnp.float32)
        g_rows[row : row + piece.shape[0], :] = grads.astype(jnp.bfloat16)
        row += piece.shape[0]
    x_rows = jnp.concatenate([piece[:, :model_width] for piece in pieces], axis=0)
    act_value, gate_value, up_value = hidden_grads(
        contract_inner(x_rows, w_gate[...]),
        contract_inner(x_rows, w_up[...]),
        contract_last(g_rows[...], w_down[...]),
    )
    activation[...] = act_value
    gate_grad[...] = gate_value
    up_grad[...] = up_value
    sums = contract_last(gate_value, w_gate[...]) + contract_last(up_value, w_up[...])
    half = own_sums.shape[0]
    own_sums[...] = sums[:half].astype(jnp.bfloat16)
    sib_sums[...] = sums[half:].astype(jnp.bfloat16)


def expert_pass(pieces, weights, mine):
    rows = sum(piece.shape[0] for piece in pieces)
    model_width, hidden_units = weights[0].shape
    hidden = jax.ShapeDtypeStruct((rows, hidden_units), jnp.bfloat16)
    wide = jax.ShapeDtypeStruct((rows, model_width), jnp.bfloat16)
    part = jax.ShapeDtypeStruct((rows // 2, model_width), jnp.bfloat16)
    in_vmem = pl.BlockSpec(memory_space=pltpu.VMEM)
    return pl.pallas_call(
        functools.partial(pass_kernel, len(pieces)),
        out_shape=(hidden, hidden, hidden, wide, part, part),
        in_specs=[in_vmem] * (len(pieces) + 4),
        out_specs=(in_vmem,) * 6,
        cost_estimate=pl.CostEstimate(
            flops=10 * rows * model_width * hidden_units,
            bytes_accessed=6 * model_width * hidden_units,
            transcendentals=rows * hidden_units,
        ),
        compiler_params=pltpu.CompilerParams(vmem_limit_bytes=24 << 20),
    )(*pieces, *weights, mine)


def outer_kernel(left_count, right_count, steps, *refs):
    lefts, refs = refs[:left_count], refs[left_count:]
    each = (len(refs) - 2 * right_count - 1) // right_count
    rights, refs = refs[: each * right_count], refs[each * right_count :]
    outs, held, copied = refs[:right_count], refs[right_count:-1], refs[-1]
    width = outs[0].shape[0] // steps
    copies = []
    for step in range(steps):
        block = pl.ds(step * width, width)
        left = jnp.concatenate([value[:, block] for value in lefts], axis=0)
        for i in range(right_count):
            right = [value[...] for value in rights[i * each : (i + 1) * each]]
            held[i][block, :] = contract_first(left, jnp.concatenate(right, axis=0))
            copies.append(
                pltpu.make_async_copy(
                    held[i].at[block, :], outs[i].at[block, :], copied.at[len(copies)]
                )
            )
            copies[-1].start()
    for copy in copies:
        copy.wait()


def outer_sums(lefts, left_width, rights, steps):
    rows = sum(value.shape[0] for value in lefts)
    right_width = rights[0][0].shape[1]
    shape = (left_width, right_width)
    values = list(lefts) + [value for right in rights for value in right]
    return pl.pallas_call(
        functools.partial(outer_kernel, len(lefts), len(rights), steps),
        out_shape=[jax.ShapeDtypeStruct(shape, jnp.float32)] * len(rights),
        in_specs=[pl.BlockSpec(memory_space=pltpu.VMEM)] * len(values),
        out_specs=[pl.BlockSpec(memory_space=pltpu.HBM)] * len(rights),
        scratch_shapes=[pltpu.VMEM(shape, jnp.float32)] * len(rights)
        + [pltpu.SemaphoreType.DMA((steps * len(rights),))],
        cost_estimate=pl.CostEstimate(
            flops=2 * rows * left_width * right_width * len(rights),
            bytes_accessed=4 * left_width * right_width * len(rights),
            transcendentals=0,
        ),
        compiler_params=pltpu.CompilerParams(vmem_limit_bytes=24 << 20),
    )(*values)


def total(*values):
    return sum(value.astype(jnp.float32) for value in values).astype(jnp.bfloat16)


def add(left, right):
    return total(left, right)


def all_rows(tokens, out_grad, expert_ids, gate_values, w_gate, w_up, w_down):
    expert_count = lax.axis_size("expert")
    device_count = lax.axis_size("dp") * expert_count
    model_width, hidden_units = w_gate.shape[1:]
    top = device_count // 2
    side, cross, core = (2, top), (top, 2), (1, 1)
    both = (2 + top, 2 + top)
    line = top // 4

    def go(value, masks):
        return swap(value, masks, device_count)

    def along(value, step):
        return go(value, (4 * step, 4 * step))

    rows = routed_rows(tokens, out_grad, expert_ids, gate_values, expert_count)
    lines = [rows] + [along(rows, i) for i in range(1, line)]
    weights = bring((w_gate[0], w_up[0], w_down[0]))
    mine = own_columns(expert_count, rows.shape[1] - 2 * model_width)
    join = lambda *values: jnp.concatenate(values, axis=0)
    rest = join(*lines[1:])
    own = join(rows, rest)
    own_side, rest_side = go(rows, side), go(rest, side)
    early = [own, join(own_side, rest_side)]
    crossing = (rows, rest, own_side, rest_side)
    crossed = [go(part, cross) for part in crossing]
    late = [join(*crossed[:2]), join(*crossed[2:])]
    early_sib = [go(part, core) for part in early]
    early_out = expert_pass(early + early_sib, weights, mine)
    late, _ = lax.optimization_barrier((late, early_out[0]))
    late_sib = [go(part, core) for part in late]
    late_out = expert_pass(late + late_sib, weights, mine)
    half = early_out[4].shape[0] // 2
    early_sums = add(early_out[4], go(early_out[5], core))
    sided = go(early_sums[half:], side)
    late_sums = add(late_out[4], go(late_out[5], core))
    crossed = go(late_sums[:half], cross)
    returned = go(late_sums[half:], both)
    acts, gates, ups, g_rows = zip(early_out[:4], late_out[:4])
    pieces = early + early_sib + late + late_sib
    grad_gate, grad_up = outer_sums(pieces, model_width, (gates, ups), 8)
    crossed, grad_gate, grad_up = lax.optimization_barrier((crossed, grad_gate, grad_up))
    sums = total(early_sums[:half], sided, crossed, returned)
    parts = jnp.split(sums, line, axis=0)
    back = [along(parts[i], i) for i in range(1, line)]
    (grad_down,) = outer_sums(acts, hidden_units, (g_rows,), 4)
    return total(parts[0], *back), grad_gate[None], grad_up[None], grad_down[None]


def slot_table(expert_ids, gate_values, expert_count, capacity):
    tok_rows, top_count = expert_ids.shape
    flat_ids = expert_ids.reshape(-1)
    onehot = (flat_ids[:, None] == jnp.arange(expert_count, dtype=jnp.int32)[None, :]).astype(
        jnp.int32
    )
    before = jnp.cumsum(onehot, axis=0) - onehot
    slot_rank = jnp.sum(before * onehot, axis=1)
    slot_index = flat_ids * capacity + slot_rank
    slot_hits = (
        slot_index[:, None] == jnp.arange(expert_count * capacity, dtype=jnp.int32)[None, :]
    ).astype(jnp.float32)
    owner_row = jnp.arange(tok_rows * top_count, dtype=jnp.int32) // top_count
    token_hits = (owner_row[:, None] == jnp.arange(tok_rows, dtype=jnp.int32)[None, :]).astype(
        jnp.float32
    )
    weighted = slot_hits * gate_values.reshape(-1)[:, None]
    return jnp.dot(weighted.T, token_hits, precision=lax.Precision.HIGHEST)


def slot_rows(tokens, out_grad, expert_ids, gate_values, w_gate, w_up, w_down):
    expert_count = lax.axis_size("expert")
    _, model_width = tokens.shape
    capacity = slots_of(expert_ids.shape, expert_count)
    slot_count = expert_count * capacity
    gate_table = slot_table(expert_ids, gate_values, expert_count, capacity)
    pick_table = (gate_table > 0.0).astype(jnp.float32)

    def to_experts(rows):
        return lax.all_to_all(
            rows.reshape(expert_count, capacity, model_width),
            "expert",
            split_axis=0,
            concat_axis=0,
            tiled=True,
        ).reshape(slot_count, model_width)

    sent_rows = contract_inner(pick_table.astype(jnp.bfloat16), tokens).astype(jnp.bfloat16)
    sent_grads = jnp.dot(
        gate_table, out_grad.astype(jnp.float32), precision=lax.Precision.HIGHEST
    ).astype(jnp.bfloat16)
    x_rows = lax.all_gather(to_experts(sent_rows), "dp", axis=0, tiled=True)
    g_rows = lax.all_gather(to_experts(sent_grads), "dp", axis=0, tiled=True)
    activation, gate_grad, up_grad = hidden_grads(
        contract_inner(x_rows, w_gate[0]),
        contract_inner(x_rows, w_up[0]),
        contract_last(g_rows, w_down[0]),
    )
    sums = contract_last(gate_grad, w_gate[0]) + contract_last(up_grad, w_up[0])
    own_sums = lax.psum_scatter(
        sums.astype(jnp.bfloat16), "dp", scatter_dimension=0, tiled=True
    )
    back_rows = to_experts(own_sums).astype(jnp.float32)
    token_grad = jnp.dot(pick_table.T, back_rows, precision=lax.Precision.HIGHEST)
    grad_gate = contract_first(x_rows, gate_grad)
    grad_up = contract_first(x_rows, up_grad)
    grad_down = contract_first(activation, g_rows)
    return token_grad.astype(jnp.bfloat16), grad_gate[None], grad_up[None], grad_down[None]


def slots_of(ids_shape, expert_count):
    return 2 * ids_shape[0] * ids_shape[1] // expert_count


def solution(mesh):
    dp_count, expert_count = mesh.shape["dp"], mesh.shape["expert"]
    device_count = dp_count * expert_count

    def shards(tokens, out_grad, expert_ids, gate_values, w_gate, w_up, w_down):
        capacity = slots_of(expert_ids.shape, expert_count)
        paired = device_count >= 8 and device_count & (device_count - 1) == 0
        every_row = paired and expert_count * capacity >= expert_count * tokens.shape[0]
        body = all_rows if every_row else slot_rows
        return body(tokens, out_grad, expert_ids, gate_values, w_gate, w_up, w_down)

    split = P(AXES, None)
    return jax.shard_map(
        shards,
        mesh=mesh,
        in_specs=(split, split, split, split)
        + (P("expert", None, "dp"), P("expert", None, "dp"), P("expert", "dp", None)),
        out_specs=(split, P("expert", None, "dp"), P("expert", None, "dp"), P("expert", "dp", None)),
        check_vma=False,
    )
```

```python
import functools

import jax
import jax.numpy as jnp
from jax import lax
from jax.experimental import pallas as pl
from jax.experimental.pallas import tpu as pltpu
from jax.sharding import PartitionSpec as P


AXES = ("dp", "expert")


def contract_last(left_op, right_op):
    return lax.dot_general(
        left_op, right_op, (((1,), (1,)), ((), ())), preferred_element_type=jnp.float32
    )


def contract_first(left_op, right_op):
    return lax.dot_general(
        left_op, right_op, (((0,), (0,)), ((), ())), preferred_element_type=jnp.float32
    )


def contract_inner(left_op, right_op):
    return jnp.dot(left_op, right_op, preferred_element_type=jnp.float32)


def hidden_grads(gate_pre, up_pre, act_grad):
    sigmoid_val = jax.nn.sigmoid(gate_pre)
    silu_val = gate_pre * sigmoid_val
    activation = (silu_val * up_pre).astype(jnp.bfloat16)
    up_grad = (act_grad * silu_val).astype(jnp.bfloat16)
    gate_grad = (act_grad * up_pre * sigmoid_val * (1.0 + gate_pre * (1.0 - sigmoid_val))).astype(
        jnp.bfloat16
    )
    return activation, gate_grad, up_grad


def swap(value, masks, device_count):
    even, odd = masks
    pairs = [(i, i ^ (odd if i % 2 else even)) for i in range(device_count)]
    return lax.ppermute(value, AXES, pairs)


def row_kernel(expert_count, tokens, out_grad, expert_ids, gate_values, rows, ids_held,
               values_held, copied):
    model_width = tokens.shape[1]
    gate_width = rows.shape[1] - 2 * model_width
    moves = (
        (expert_ids, ids_held),
        (gate_values, values_held),
        (tokens, rows.at[:, pl.ds(0, model_width)]),
        (out_grad, rows.at[:, pl.ds(model_width, model_width)]),
    )
    copies = [
        pltpu.make_async_copy(source, target, copied.at[i])
        for i, (source, target) in enumerate(moves)
    ]
    for copy in copies:
        copy.start()
    copies[0].wait()
    copies[1].wait()
    column = lax.broadcasted_iota(jnp.int32, (tokens.shape[0], gate_width), 1)
    expert = lax.rem(column, expert_count)
    ids, values = ids_held[...], values_held[...]
    weight = jnp.zeros(column.shape, jnp.float32)
    for k in range(ids.shape[1]):
        weight = weight + jnp.where(ids[:, k : k + 1] == expert, values[:, k : k + 1], 0.0)
    high = weight.astype(jnp.bfloat16).astype(jnp.float32)
    middle = (weight - high).astype(jnp.bfloat16).astype(jnp.float32)
    low = weight - high - middle
    place = lax.div(column, expert_count)
    piece = jnp.where(place == 0, high, jnp.where(place == 1, middle, low))
    piece = jnp.where(place < 3, piece, 0.0)
    rows[:, 2 * model_width :] = piece.astype(jnp.bfloat16)
    copies[2].wait()
    copies[3].wait()


def in_hbm(*values):
    return [pltpu.with_memory_space_constraint(value, pltpu.HBM) for value in values]


def routed_rows(tokens, out_grad, expert_ids, gate_values, expert_count):
    gate_width = -(-3 * expert_count // 128) * 128
    return pl.pallas_call(
        functools.partial(row_kernel, expert_count),
        out_shape=jax.ShapeDtypeStruct(
            (tokens.shape[0], 2 * tokens.shape[1] + gate_width), jnp.bfloat16
        ),
        in_specs=[pl.BlockSpec(memory_space=pltpu.HBM)] * 4,
        out_specs=pl.BlockSpec(memory_space=pltpu.VMEM),
        scratch_shapes=[
            pltpu.VMEM(expert_ids.shape, expert_ids.dtype),
            pltpu.VMEM(gate_values.shape, gate_values.dtype),
            pltpu.SemaphoreType.DMA((4,)),
        ],
        compiler_params=pltpu.CompilerParams(vmem_limit_bytes=4 << 20),
        name="routed_rows",
    )(*in_hbm(tokens, out_grad, expert_ids, gate_values))


def column_kernel(expert_count, mine):
    column = lax.broadcasted_iota(jnp.int32, mine.shape, 1)
    own = lax.rem(column, expert_count) == lax.axis_index("expert")
    mine[...] = jnp.where(own & (column < 3 * expert_count), 1.0, 0.0)


def own_columns(expert_count, gate_width):
    return pl.pallas_call(
        functools.partial(column_kernel, expert_count),
        out_shape=jax.ShapeDtypeStruct((1, gate_width), jnp.float32),
        out_specs=pl.BlockSpec(memory_space=pltpu.VMEM),
        cost_estimate=pl.CostEstimate(flops=8 << 30, bytes_accessed=0, transcendentals=0),
        compiler_params=pltpu.CompilerParams(vmem_limit_bytes=1 << 20),
        name="own_columns",
    )()


def pass_kernel(piece_count, *refs):
    pieces, (w_gate, w_up, w_down, mine), outs = (
        refs[:piece_count],
        refs[piece_count : piece_count + 4],
        refs[piece_count + 4 :],
    )
    activation, gate_grad, up_grad, g_rows, own_sums, sib_sums = outs
    model_width = w_gate.shape[0]
    row = 0
    for piece in pieces:
        weights = piece[:, 2 * model_width :].astype(jnp.float32)
        gate = jnp.sum(weights * mine[...], axis=1, keepdims=True)
        grads = gate * piece[:, model_width : 2 * model_width].astype(jnp.float32)
        g_rows[row : row + piece.shape[0], :] = grads.astype(jnp.bfloat16)
        row += piece.shape[0]
    x_rows = jnp.concatenate([piece[:, :model_width] for piece in pieces], axis=0)
    act_value, gate_value, up_value = hidden_grads(
        contract_inner(x_rows, w_gate[...]),
        contract_inner(x_rows, w_up[...]),
        contract_last(g_rows[...], w_down[...]),
    )
    activation[...] = act_value
    gate_grad[...] = gate_value
    up_grad[...] = up_value
    sums = contract_last(gate_value, w_gate[...]) + contract_last(up_value, w_up[...])
    half = own_sums.shape[0]
    own_sums[...] = sums[:half].astype(jnp.bfloat16)
    sib_sums[...] = sums[half:].astype(jnp.bfloat16)


def expert_pass(pieces, weights, mine):
    rows = sum(piece.shape[0] for piece in pieces)
    model_width, hidden_units = weights[0].shape
    hidden = jax.ShapeDtypeStruct((rows, hidden_units), jnp.bfloat16)
    wide = jax.ShapeDtypeStruct((rows, model_width), jnp.bfloat16)
    part = jax.ShapeDtypeStruct((rows // 2, model_width), jnp.bfloat16)
    in_vmem = pl.BlockSpec(memory_space=pltpu.VMEM)
    return pl.pallas_call(
        functools.partial(pass_kernel, len(pieces)),
        out_shape=(hidden, hidden, hidden, wide, part, part),
        in_specs=[in_vmem] * (len(pieces) + 4),
        out_specs=(in_vmem,) * 6,
        cost_estimate=pl.CostEstimate(
            flops=10 * rows * model_width * hidden_units,
            bytes_accessed=6 * model_width * hidden_units,
            transcendentals=rows * hidden_units,
        ),
        compiler_params=pltpu.CompilerParams(vmem_limit_bytes=24 << 20),
    )(*pieces, *weights, mine)


def outer_kernel(left_count, right_count, steps, *refs):
    lefts, refs = refs[:left_count], refs[left_count:]
    each = (len(refs) - 2 * right_count - 1) // right_count
    rights, refs = refs[: each * right_count], refs[each * right_count :]
    outs, held, copied = refs[:right_count], refs[right_count:-1], refs[-1]
    width = outs[0].shape[0] // steps
    copies = []
    for step in range(steps):
        block = pl.ds(step * width, width)
        left = jnp.concatenate([value[:, block] for value in lefts], axis=0)
        for i in range(right_count):
            right = [value[...] for value in rights[i * each : (i + 1) * each]]
            held[i][block, :] = contract_first(left, jnp.concatenate(right, axis=0))
            copies.append(
                pltpu.make_async_copy(
                    held[i].at[block, :], outs[i].at[block, :], copied.at[len(copies)]
                )
            )
            copies[-1].start()
    for copy in copies:
        copy.wait()


def outer_sums(lefts, left_width, rights, steps):
    rows = sum(value.shape[0] for value in lefts)
    right_width = rights[0][0].shape[1]
    shape = (left_width, right_width)
    values = list(lefts) + [value for right in rights for value in right]
    return pl.pallas_call(
        functools.partial(outer_kernel, len(lefts), len(rights), steps),
        out_shape=[jax.ShapeDtypeStruct(shape, jnp.float32)] * len(rights),
        in_specs=[pl.BlockSpec(memory_space=pltpu.VMEM)] * len(values),
        out_specs=[pl.BlockSpec(memory_space=pltpu.HBM)] * len(rights),
        scratch_shapes=[pltpu.VMEM(shape, jnp.float32)] * len(rights)
        + [pltpu.SemaphoreType.DMA((steps * len(rights),))],
        cost_estimate=pl.CostEstimate(
            flops=2 * rows * left_width * right_width * len(rights),
            bytes_accessed=4 * left_width * right_width * len(rights),
            transcendentals=0,
        ),
        compiler_params=pltpu.CompilerParams(vmem_limit_bytes=24 << 20),
    )(*values)


def total(*values):
    return sum(value.astype(jnp.float32) for value in values).astype(jnp.bfloat16)


def add(left, right):
    return total(left, right)


def all_rows(tokens, out_grad, expert_ids, gate_values, w_gate, w_up, w_down):
    expert_count = lax.axis_size("expert")
    device_count = lax.axis_size("dp") * expert_count
    model_width, hidden_units = w_gate.shape[1:]
    top = device_count // 2
    side, cross, core = (2, top), (top, 2), (1, 1)
    both = (2 + top, 2 + top)
    line = top // 4

    def go(value, masks):
        return swap(value, masks, device_count)

    def along(value, step):
        return go(value, (4 * step, 4 * step))

    rows = routed_rows(tokens, out_grad, expert_ids, gate_values, expert_count)
    lines = [rows] + [along(rows, i) for i in range(1, line)]
    weights = (w_gate[0], w_up[0], w_down[0])
    mine = own_columns(expert_count, rows.shape[1] - 2 * model_width)
    join = lambda *values: jnp.concatenate(values, axis=0)
    rest = join(*lines[1:])
    own = join(rows, rest)
    own_side, rest_side = go(rows, side), go(rest, side)
    early = [own, join(own_side, rest_side)]
    crossing = (rows, rest, own_side, rest_side)
    crossed = [go(part, cross) for part in crossing]
    late = [join(*crossed[:2]), join(*crossed[2:])]
    early_sib = [go(part, core) for part in early]
    early_out = expert_pass(early + early_sib, weights, mine)
    late, _ = lax.optimization_barrier((late, early_out[0]))
    late_sib = [go(part, core) for part in late]
    late_out = expert_pass(late + late_sib, weights, mine)
    half = early_out[4].shape[0] // 2
    early_sums = add(early_out[4], go(early_out[5], core))
    sided = go(early_sums[half:], side)
    late_sums = add(late_out[4], go(late_out[5], core))
    crossed = go(late_sums[:half], cross)
    returned = go(late_sums[half:], both)
    acts, gates, ups, g_rows = zip(early_out[:4], late_out[:4])
    pieces = early + early_sib + late + late_sib
    grad_gate, grad_up = outer_sums(pieces, model_width, (gates, ups), 8)
    crossed, grad_gate, grad_up = lax.optimization_barrier((crossed, grad_gate, grad_up))
    sums = total(early_sums[:half], sided, crossed, returned)
    parts = jnp.split(sums, line, axis=0)
    back = [along(parts[i], i) for i in range(1, line)]
    (grad_down,) = outer_sums(acts, hidden_units, (g_rows,), 4)
    return total(parts[0], *back), grad_gate[None], grad_up[None], grad_down[None]


def slot_table(expert_ids, gate_values, expert_count, capacity):
    tok_rows, top_count = expert_ids.shape
    flat_ids = expert_ids.reshape(-1)
    onehot = (flat_ids[:, None] == jnp.arange(expert_count, dtype=jnp.int32)[None, :]).astype(
        jnp.int32
    )
    before = jnp.cumsum(onehot, axis=0) - onehot
    slot_rank = jnp.sum(before * onehot, axis=1)
    slot_index = flat_ids * capacity + slot_rank
    slot_hits = (
        slot_index[:, None] == jnp.arange(expert_count * capacity, dtype=jnp.int32)[None, :]
    ).astype(jnp.float32)
    owner_row = jnp.arange(tok_rows * top_count, dtype=jnp.int32) // top_count
    token_hits = (owner_row[:, None] == jnp.arange(tok_rows, dtype=jnp.int32)[None, :]).astype(
        jnp.float32
    )
    weighted = slot_hits * gate_values.reshape(-1)[:, None]
    return jnp.dot(weighted.T, token_hits, precision=lax.Precision.HIGHEST)


def slot_rows(tokens, out_grad, expert_ids, gate_values, w_gate, w_up, w_down):
    expert_count = lax.axis_size("expert")
    _, model_width = tokens.shape
    capacity = slots_of(expert_ids.shape, expert_count)
    slot_count = expert_count * capacity
    gate_table = slot_table(expert_ids, gate_values, expert_count, capacity)
    pick_table = (gate_table > 0.0).astype(jnp.float32)

    def to_experts(rows):
        return lax.all_to_all(
            rows.reshape(expert_count, capacity, model_width),
            "expert",
            split_axis=0,
            concat_axis=0,
            tiled=True,
        ).reshape(slot_count, model_width)

    sent_rows = contract_inner(pick_table.astype(jnp.bfloat16), tokens).astype(jnp.bfloat16)
    sent_grads = jnp.dot(
        gate_table, out_grad.astype(jnp.float32), precision=lax.Precision.HIGHEST
    ).astype(jnp.bfloat16)
    x_rows = lax.all_gather(to_experts(sent_rows), "dp", axis=0, tiled=True)
    g_rows = lax.all_gather(to_experts(sent_grads), "dp", axis=0, tiled=True)
    activation, gate_grad, up_grad = hidden_grads(
        contract_inner(x_rows, w_gate[0]),
        contract_inner(x_rows, w_up[0]),
        contract_last(g_rows, w_down[0]),
    )
    sums = contract_last(gate_grad, w_gate[0]) + contract_last(up_grad, w_up[0])
    own_sums = lax.psum_scatter(
        sums.astype(jnp.bfloat16), "dp", scatter_dimension=0, tiled=True
    )
    back_rows = to_experts(own_sums).astype(jnp.float32)
    token_grad = jnp.dot(pick_table.T, back_rows, precision=lax.Precision.HIGHEST)
    grad_gate = contract_first(x_rows, gate_grad)
    grad_up = contract_first(x_rows, up_grad)
    grad_down = contract_first(activation, g_rows)
    return token_grad.astype(jnp.bfloat16), grad_gate[None], grad_up[None], grad_down[None]


def slots_of(ids_shape, expert_count):
    return 2 * ids_shape[0] * ids_shape[1] // expert_count


def solution(mesh):
    dp_count, expert_count = mesh.shape["dp"], mesh.shape["expert"]
    device_count = dp_count * expert_count

    def shards(tokens, out_grad, expert_ids, gate_values, w_gate, w_up, w_down):
        capacity = slots_of(expert_ids.shape, expert_count)
        paired = device_count >= 8 and device_count & (device_count - 1) == 0
        every_row = paired and expert_count * capacity >= expert_count * tokens.shape[0]
        body = all_rows if every_row else slot_rows
        return body(tokens, out_grad, expert_ids, gate_values, w_gate, w_up, w_down)

    split = P(AXES, None)
    return jax.shard_map(
        shards,
        mesh=mesh,
        in_specs=(split, split, split, split)
        + (P("expert", None, "dp"), P("expert", None, "dp"), P("expert", "dp", None)),
        out_specs=(split, P("expert", None, "dp"), P("expert", None, "dp"), P("expert", "dp", None)),
        check_vma=False,
    )
```
